32 devices in a mesh: groups: 2 (over y), ctx: 8 (over z, x), head: 2 (over core).
Axes of the slice: x: 2, y: 2, z: 4, core: 2. Of those that a mesh axis runs over, the one named last changes fastest.
Arguments:
- queries: bfloat16 [16, 128, 64, 192], P(('groups', 'ctx'), None, 'head'), parts along dimension 0, may hold values from -360 to 360
- latent_pages: bfloat16 [16, 8, 64, 576], P(('groups', 'ctx'), 'head'), parts along dimension 0, may hold values from -6 to 6
- page_scales: bfloat16 [16, 8, 4, 64], P(('groups', 'ctx'), 'head'), parts along dimension 0, may hold values from 0.5 to 2
- page_table: int32 [16, 8], P(('groups', 'ctx')), parts along dimension 0, may hold values from 0 to 7, each once within a row
- lengths: int32 [16], P(('groups', 'ctx')), parts along dimension 0, may hold values from 128 to 512, as said below
- w_keys: bfloat16 [512, 64, 128], P('ctx', 'head'), may hold values from -0.5 to 0.5
- w_values: bfloat16 [512, 64, 128], P('ctx', 'head'), may hold values from -1 to 1
Outputs:
- attended: bfloat16 [16, 128, 64, 128], P(('groups', 'ctx'), None, 'head'), parts along dimension 0
The draws below stay inside these ranges and needn't reach their ends.
There are 2 independent parts, one for each index of `groups`. The reference program is written for one: setup_inputs(seed, part) draws one part's arguments, and reference() takes and returns one part's arrays. A program takes and returns all parts, laid end to end along the dimension named above; an argument that names none is the same for every part. Nothing has to cross between parts.
Inputs may be any that keep to these rules, and one draw needn't show every extreme that they name: `page_table`: each row is a permutation of 0 to 7. `lengths`: a length counts the cached tokens and the 128 rows of the span, which take the last positions; the longest request of a part has exactly 512 tokens.
All inputs are finite; a program needn't handle non-finite values.
Results may differ from the reference program's by a relative error of at most 0.0084.
Values may be sent and summed in bfloat16 or wider, within the bound.
A program may use at most 64 MiB of HBM per device.

```python
import math
import jax
import jax.numpy as jnp
from jax import lax

HEADS = 64
NOPE = 128
ROPE = 64
VDIM = 128
LATENT = 512
GROUPS = 4
PAGE = 64
SPAN = 128
PAGES_REQ = 8
REQS = 8


def draw_latent_pages(key, part):
    code_key = jax.random.fold_in(key, 202)
    rope_key = jax.random.fold_in(key, 303)
    code_values = jnp.clip(jax.random.normal(code_key, (REQS, PAGES_REQ, PAGE, LATENT), jnp.float32), -6.0, 6.0)
    rotary = jnp.clip(jax.random.normal(rope_key, (REQS, PAGES_REQ, PAGE, ROPE), jnp.float32), -4.0, 4.0)
    return jnp.concatenate([code_values, rotary], axis=-1).astype(jnp.bfloat16)


def draw_queries(key, part):
    full_shape = (REQS, SPAN, HEADS, NOPE + ROPE)
    main_key = jax.random.fold_in(key, 404)
    drawn = jnp.clip(jax.random.normal(main_key, full_shape, jnp.float32), -6.0, 6.0)
    return drawn.astype(jnp.bfloat16)


def draw_lengths(key, part):
    longest_tokens = PAGES_REQ * PAGE
    reach = longest_tokens - SPAN + 1
    first_key = jax.random.fold_in(key, 606)
    second_key = jax.random.fold_in(key, 707)
    third_key = jax.random.fold_in(key, 808)
    first_draw = jax.random.randint(first_key, (REQS,), 0, reach, jnp.int32)
    second_draw = jax.random.randint(second_key, (REQS,), 0, reach, jnp.int32)
    extra_tokens = first_draw * second_draw // reach
    chosen_request = jax.random.randint(third_key, (), 0, REQS, jnp.int32)
    result = SPAN + extra_tokens
    return result.at[chosen_request].set(longest_tokens)


def steps_of(stream_key, dims, shards, least, top_value):
    loudness, own = 1.0, jax.random.fold_in(stream_key, 6)
    for axis_at, parts in shards:
        draws = jnp.exp(jax.random.uniform(jax.random.fold_in(own, axis_at), (parts,), jnp.float32, least / len(shards), top_value / len(shards)))
        loudness = loudness * jnp.repeat(draws, dims[axis_at] // parts).reshape([-1 if axis == axis_at else 1 for axis in range(len(dims))])
    return loudness


def gaussian(rng, extent, width, limit, cuts=(), dtype=jnp.bfloat16):
    array = width * jax.random.normal(rng, extent, jnp.float32)
    if cuts:
        array = array * steps_of(rng, extent, cuts, -0.22, 0.18)
    return jnp.clip(array, -limit, limit).astype(dtype)


def setup_inputs(seed: int = 0, part: int = 0) -> dict:
    seeds = jax.random.split(jax.random.key(seed), 8)
    own_keys = jax.random.split(jax.random.fold_in(seeds[7], part), 8)
    queries = draw_queries(jax.random.fold_in(jax.random.fold_in(seeds[7], part), 71), part)
    latent_pages = draw_latent_pages(jax.random.fold_in(jax.random.fold_in(seeds[7], part), 71), part)
    page_scales = jnp.clip(jnp.exp(math.log(2.0) - 1.3862944 * jax.random.uniform(own_keys[2], (REQS, PAGES_REQ, GROUPS, PAGE), jnp.float32) ** steps_of(own_keys[2], (REQS, PAGES_REQ, GROUPS, PAGE), ((0, 8), (1, 2)), -0.2, 0.2)), 0.5, 2.0).astype(jnp.bfloat16)
    page_table = jax.vmap(lambda own: jax.random.permutation(own, PAGES_REQ))(jax.random.split(own_keys[3], REQS)).reshape((REQS, PAGES_REQ)).astype(jnp.int32)
    lengths = draw_lengths(jax.random.fold_in(jax.random.fold_in(seeds[7], part), 71), part)
    w_keys = gaussian(seeds[5], (LATENT, HEADS, NOPE), (LATENT // 4) ** -0.5, 0.5, ((0, 8), (1, 2)))
    w_values = gaussian(seeds[6], (LATENT, HEADS, VDIM), (LATENT // 16) ** -0.5, 1.0, ((0, 8), (1, 2)))
    return {"queries": queries, "latent_pages": latent_pages, "page_scales": page_scales, "page_table": page_table, "lengths": lengths, "w_keys": w_keys, "w_values": w_values}


def one_request(span_query, pool_pages, pool_scales, pool_table, length_one, w_keys, w_values):
    ordered = jnp.take(pool_pages, pool_table.astype(jnp.int32), axis=0)
    ordered_scales = jnp.take(pool_scales, pool_table.astype(jnp.int32), axis=0)
    key_count = PAGES_REQ * PAGE
    code_values = ordered[:, :, :LATENT].astype(jnp.float32).reshape(PAGES_REQ, PAGE, GROUPS, LATENT // GROUPS)
    factor = jnp.swapaxes(ordered_scales, 1, 2).astype(jnp.float32)[..., None]
    latent = (code_values * factor).reshape(key_count, LATENT).astype(jnp.bfloat16)
    rotary = ordered[:, :, LATENT:].reshape(key_count, ROPE)
    key_nope = jnp.dot(latent, w_keys.reshape(LATENT, HEADS * NOPE), preferred_element_type=jnp.float32)
    key_nope = key_nope.astype(jnp.bfloat16).reshape(key_count, HEADS, NOPE)
    value_rows = jnp.dot(latent, w_values.reshape(LATENT, HEADS * VDIM), preferred_element_type=jnp.float32)
    value_rows = value_rows.astype(jnp.bfloat16).reshape(key_count, HEADS, VDIM)
    query_nope = span_query[:, :, :NOPE].astype(jnp.float32)
    query_rope = span_query[:, :, NOPE:].astype(jnp.float32)
    scores = jnp.einsum('chn,khn->hck', query_nope, key_nope.astype(jnp.float32))
    scores = scores + jnp.einsum('chr,kr->hck', query_rope, rotary.astype(jnp.float32))
    scores = scores * (1.0 / math.sqrt(NOPE + ROPE))
    row_position = lax.broadcasted_iota(jnp.int32, (SPAN, key_count), 0)
    key_position = lax.broadcasted_iota(jnp.int32, (SPAN, key_count), 1)
    visible = (key_position <= length_one.astype(jnp.int32) - SPAN + row_position)[None]
    row_top = lax.optimization_barrier(jnp.max(jnp.where(visible, scores, -jnp.inf), axis=2))
    raw_weight = jnp.where(visible, jnp.exp(scores - row_top[..., None]), 0.0)
    row_total = lax.optimization_barrier(jnp.sum(raw_weight, axis=2))
    weights = raw_weight.astype(jnp.bfloat16)
    summed = jnp.einsum('hck,khv->chv', weights.astype(jnp.float32), value_rows.astype(jnp.float32))
    return (summed / jnp.swapaxes(row_total, 0, 1)[..., None]).astype(jnp.bfloat16)

def reference(queries, latent_pages, page_scales, page_table, lengths, w_keys, w_values):

    def handle(operands):
        return one_request(operands[0], operands[1], operands[2], operands[3], operands[4], w_keys, w_values)
    return lax.map(handle, (queries, latent_pages, page_scales, page_table, lengths))
```

```python
import functools
import math

import jax
import jax.numpy as jnp
from jax import lax
from jax.experimental import pallas as pl
from jax.experimental.pallas import tpu as pltpu
from jax.sharding import PartitionSpec as P

NEGATIVE = -1e30
MESH = pl.DeviceIdType.MESH
PAIR = 2
LAG = 2


def attend_block(
    running, span_query, page_data, page_factor, first_key, row_offset, up_keys, up_values
):
    row_top, row_total, summed = running
    latent_width = up_keys.shape[0]
    group_count = page_factor.shape[1]
    page_rows = page_data.shape[1]
    key_count = page_data.shape[0] * page_rows
    head_count = span_query.shape[1]
    code_values = page_data[:, :, :latent_width].astype(jnp.float32)
    code_values = code_values.reshape(
        page_data.shape[0], page_rows, group_count, latent_width // group_count
    )
    factor = jnp.swapaxes(page_factor, 1, 2).astype(jnp.float32)[..., None]
    latent = (code_values * factor).reshape(key_count, latent_width).astype(jnp.bfloat16)
    rotary = page_data[:, :, latent_width:].reshape(key_count, -1)
    key_nope = jnp.dot(latent, up_keys, preferred_element_type=jnp.float32).astype(jnp.bfloat16)
    key_nope = key_nope.reshape(key_count, head_count, -1)
    value_rows = jnp.dot(latent, up_values, preferred_element_type=jnp.float32).astype(jnp.bfloat16)
    value_rows = value_rows.reshape(key_count, head_count, -1)
    nope_width = key_nope.shape[2]
    scores = jnp.einsum(
        "chn,khn->hck", span_query[:, :, :nope_width], key_nope, preferred_element_type=jnp.float32
    )
    scores = scores + jnp.einsum(
        "chr,kr->hck", span_query[:, :, nope_width:], rotary, preferred_element_type=jnp.float32
    )
    scores = scores * (1.0 / math.sqrt(span_query.shape[2]))
    row_position = lax.broadcasted_iota(jnp.int32, (span_query.shape[0], key_count), 0)
    key_position = first_key + lax.broadcasted_iota(jnp.int32, (span_query.shape[0], key_count), 1)
    visible = (key_position <= row_offset + row_position)[None]
    new_top = jnp.maximum(row_top, jnp.max(jnp.where(visible, scores, NEGATIVE), axis=2))
    raw_weight = jnp.where(visible, jnp.exp(scores - new_top[..., None]), 0.0)
    rescale = jnp.exp(row_top - new_top)
    row_total = row_total * rescale + jnp.sum(raw_weight, axis=2)
    weights = raw_weight.astype(jnp.bfloat16)
    summed = summed * jnp.swapaxes(rescale, 0, 1)[..., None] + jnp.einsum(
        "hck,khv->chv", weights, value_rows, preferred_element_type=jnp.float32
    )
    return (new_top, row_total, summed)


def sweep(span_query, row_offset, first_block, stop_block, fetch, up_keys, up_values):
    row_count = span_query.shape[0]
    head_count = span_query.shape[1]
    value_width = up_values.shape[1] // head_count
    initial = (
        jnp.full((head_count, row_count), NEGATIVE, jnp.float32),
        jnp.zeros((head_count, row_count), jnp.float32),
        jnp.zeros((row_count, head_count, value_width), jnp.float32),
    )

    def advance(block_index, running):
        page_data, page_factor, first_key = fetch(block_index)
        return attend_block(
            running, span_query, page_data, page_factor, first_key, row_offset, up_keys, up_values
        )

    return lax.fori_loop(first_block, stop_block, advance, initial)


def finish(row_total, summed):
    return (summed / jnp.swapaxes(row_total, 0, 1)[..., None]).astype(jnp.bfloat16)[None]


def on_device(queries, latent_pages, page_scales, page_table, lengths, w_keys, w_values):
    pool_pages, pool_scales = (
        lax.all_gather(latent_pages, "head", axis=1, tiled=True),
        lax.all_gather(page_scales, "head", axis=1, tiled=True),
    )
    full_keys, full_values = (
        lax.all_gather(w_keys, "ctx", axis=0, tiled=True),
        lax.all_gather(w_values, "ctx", axis=0, tiled=True),
    )
    latent_width = full_keys.shape[0]
    up_keys = full_keys.reshape(latent_width, -1)
    up_values = full_values.reshape(latent_width, -1)
    span_query = queries[0]
    own_pages = pool_pages[0]
    own_scales = pool_scales[0]
    own_table = page_table[0]
    row_count = span_query.shape[0]
    block_keys = 2 * own_pages.shape[1]
    own_length = lengths[0]
    block_count = (own_length + block_keys - 1) // block_keys

    def own_fetch(block_index):
        pool_slots = lax.dynamic_slice_in_dim(own_table, 2 * block_index, 2)
        return (
            jnp.take(own_pages, pool_slots, axis=0),
            jnp.take(own_scales, pool_slots, axis=0),
            block_index * block_keys,
        )

    row_top, row_total, summed = sweep(
        span_query, own_length - row_count, 0, block_count, own_fetch, up_keys, up_values
    )
    return finish(row_total, summed)


def gather_attend(
    shard_columns, q_in, k_in, t_in, w_in, out, q_rx, k_all, t_rx, w_all, rot, stage,
    own_sem, core_send, core_recv, relay_send, relay_recv, k_send, k_recv, t_send, t_recv,
    q_send, q_recv, z_send, z_recv, x_send, x_recv, f_send, f_recv, o_send, o_recv
):
    chunk_count = w_in.shape[1]
    latent_width = w_all.shape[2] * w_all.shape[3]
    nope = q_in.shape[-1]
    span = q_in.shape[-2]
    rope = nope // PAIR
    key_count = k_all.shape[1] * k_all.shape[2]
    scale = 1.0 / math.sqrt(nope + rope)
    y, ctx, core = lax.axis_index("groups"), lax.axis_index("ctx"), lax.axis_index("head")
    row, side = ctx // 2, lax.rem(ctx, 2)
    y_peer = {"groups": 1 - y}
    core_peer = {"head": 1 - core}
    x_peer = {"ctx": 2 * row + 1 - side}

    def z_index(offset):
        return 2 * lax.rem(row + offset, shard_columns) + side

    barrier = pltpu.get_barrier_semaphore()
    peers = [y_peer, core_peer, x_peer] + [{"ctx": z_index(d)} for d in range(1, shard_columns)]
    for peer in peers:
        pl.semaphore_signal(barrier, inc=1, device_id=peer, device_id_type=MESH)
    pl.semaphore_wait(barrier, len(peers))

    def remote(source, target, send, recv, peer):
        return pltpu.make_async_remote_copy(
            src_ref=source, dst_ref=target, send_sem=send, recv_sem=recv,
            device_id=peer, device_id_type=MESH,
        )

    k_copy = remote(k_in, k_all.at[y, core], k_send, k_recv, y_peer)
    t_copy = remote(t_in, t_rx, t_send, t_recv, y_peer)
    core_copy = remote(k_in, k_all.at[y, core], core_send, core_recv, core_peer)
    relay_copy = remote(
        k_all.at[1 - y, core], k_all.at[1 - y, core], relay_send, relay_recv, core_peer
    )
    k_own = pltpu.make_async_copy(k_in, k_all.at[y, core], own_sem.at[0])
    w_own = pltpu.make_async_copy(w_in.at[y], w_all.at[:, :, ctx], own_sem.at[1])

    def q_copy(c):
        return remote(q_in.at[1 - y, c], q_rx.at[c], q_send.at[c], q_recv.at[c], y_peer)

    def z_copy(c, d):
        return remote(
            w_in.at[y, c], w_all.at[c, :, ctx], z_send.at[c, d - 1], z_recv.at[c, d - 1],
            {"ctx": z_index(d)},
        )

    def x_copy(c):
        return remote(w_in.at[y, c], w_all.at[c, :, ctx], x_send.at[c], x_recv.at[c], x_peer)

    def f_copy(c, d):
        block = w_all.at[c, :, z_index(shard_columns - d)]
        return remote(block, block, f_send.at[c, d - 1], f_recv.at[c, d - 1], x_peer)

    def o_copy(c):
        return remote(stage.at[c], out.at[y, c], o_send.at[c], o_recv.at[c], y_peer)

    k_copy.start()
    t_copy.start()
    core_copy.start()
    k_own.start()
    w_own.start()

    def begin(c, carry):
        for d in range(1, shard_columns):
            z_copy(c, d).start()
        x_copy(c).start()
        q_copy(c).start()
        return carry

    lax.fori_loop(0, chunk_count, begin, 0)
    k_own.wait()
    w_own.wait()
    k_copy.wait_recv()
    relay_copy.start()
    t_copy.wait_recv()
    core_copy.wait_recv()
    relay_copy.wait_recv()
    lane = lax.broadcasted_iota(jnp.int32, (key_count, nope), 1)
    for r in range(2):
        both = k_all[r, :, :, latent_width:].reshape(key_count, nope)
        rot[r, 0] = jnp.where(lane < rope, both, jnp.zeros_like(both))
        rot[r, 1] = jnp.where(lane < rope, jnp.zeros_like(both), both)
    row_position = lax.broadcasted_iota(jnp.int32, (span, key_count), 0)

    def attend(c, request, q_ref, t_ref, put):
        latent = k_all[request, :, :, :latent_width].reshape(key_count, latent_width)
        visible = t_ref[0:1, :] <= row_position
        for h in range(PAIR):
            weight = w_all[c, h].reshape(latent_width, -1)
            up = jnp.dot(latent, weight, preferred_element_type=jnp.float32).astype(jnp.bfloat16)
            keys = jnp.concatenate([up[:, :nope], rot[request, h]], axis=1)
            query = jnp.concatenate([q_ref[h], q_ref[PAIR]], axis=1)
            scores = lax.dot_general(
                query, keys, (((1,), (1,)), ((), ())), preferred_element_type=jnp.float32
            )
            scores = jnp.where(visible, scores * scale, NEGATIVE)
            top = jnp.max(scores, axis=1, keepdims=True)
            raw = jnp.where(visible, jnp.exp(scores - top), 0.0)
            total = jnp.sum(raw, axis=1, keepdims=True)
            summed = jnp.dot(
                raw.astype(jnp.bfloat16), up[:, nope:], preferred_element_type=jnp.float32
            )
            put(h, (summed / total).astype(jnp.bfloat16))

    def advance(c, carry):
        @pl.when(c < chunk_count)
        def _():
            for d in range(1, shard_columns):
                z_copy(c, d).wait_recv()
                f_copy(c, d).start()

        @pl.when(c >= LAG)
        def _():
            b = c - LAG
            x_copy(b).wait_recv()
            for d in range(1, shard_columns):
                f_copy(b, d).wait_recv()
            q_copy(b).wait_recv()

            def put_stage(h, value):
                stage[b, h] = value

            def put_out(h, value):
                out[y, b, h] = value

            attend(b, 1 - y, q_rx.at[b], t_rx, put_stage)
            attend(b, y, q_in.at[y, b], t_in, put_out)
            o_copy(b).start()

        return carry

    lax.fori_loop(0, chunk_count + LAG, advance, 0)
    k_copy.wait_send()
    t_copy.wait_send()
    core_copy.wait_send()
    relay_copy.wait_send()

    def end(c, carry):
        q_copy(c).wait_send()
        x_copy(c).wait_send()
        for d in range(1, shard_columns):
            z_copy(c, d).wait_send()
            f_copy(c, d).wait_send()
        o_copy(c).wait()
        return carry

    lax.fori_loop(0, chunk_count, end, 0)


def shared_on_device(
    shards, queries, latent_pages, page_scales, page_table, lengths, w_keys, w_values
):
    _, span, heads, _ = queries.shape
    latent_rows, _, nope = w_keys.shape
    _, slots, page, width = latent_pages.shape
    latent_width = latent_rows * shards
    rope = width - latent_width
    groups = page_scales.shape[2]
    chunks = heads // (2 * PAIR)
    keys = slots * page
    columns = shards // 2
    w_in = jnp.concatenate([jnp.swapaxes(w_keys, 0, 1), jnp.swapaxes(w_values, 0, 1)], axis=-1)
    w_in = w_in.reshape(2, chunks, PAIR, latent_rows, 2 * nope)
    query = queries[0]
    q_nope = jnp.swapaxes(query[:, :, :nope], 0, 1).reshape(2, chunks, PAIR, span, nope)
    q_rope = query[:, :, nope:].reshape(span, heads // PAIR, nope)
    q_rope = jnp.swapaxes(q_rope, 0, 1).reshape(2, chunks, 1, span, nope)
    q_in = jnp.concatenate([q_nope, q_rope], axis=2)
    codes = latent_pages[0, :, :, :latent_width].astype(jnp.float32)
    codes = codes.reshape(slots, page, groups, latent_width // groups)
    factor = jnp.swapaxes(page_scales[0], 1, 2).astype(jnp.float32)[..., None]
    latent = (codes * factor).reshape(keys, latent_width).astype(jnp.bfloat16)
    rotary = latent_pages[0, :, :, latent_width:].reshape(keys, rope)
    k_in = jnp.concatenate([latent, rotary, rotary], axis=1)
    pool = page_table.shape[1]
    places = jnp.arange(pool, dtype=jnp.int32)
    order = jnp.sum(jnp.where(page_table[0][:, None] == places[None], places[:, None], 0), axis=0)
    first = order[:, None] * page + jnp.arange(page, dtype=jnp.int32)[None]
    first = first.reshape(1, pool * page) - (lengths[0] - span)
    t_in = jnp.broadcast_to(first, (8, pool * page))
    dma, vmem = pltpu.SemaphoreType.DMA, pltpu.VMEM
    bf16 = jnp.bfloat16
    out = pl.pallas_call(
        functools.partial(gather_attend, columns),
        out_shape=jax.ShapeDtypeStruct((2, chunks, PAIR, span, nope), bf16),
        in_specs=[pl.BlockSpec(memory_space=vmem)] * 4,
        out_specs=pl.BlockSpec(memory_space=vmem),
        scratch_shapes=[
            vmem((chunks, PAIR + 1, span, nope), bf16),
            vmem((2, 2, keys, k_in.shape[1]), bf16),
            vmem(t_in.shape, jnp.int32),
            vmem((chunks, PAIR, shards, latent_rows, 2 * nope), bf16),
            vmem((2, 2, 2 * keys, nope), bf16),
            vmem((chunks, PAIR, span, nope), bf16),
            dma((2,)), dma, dma, dma, dma, dma, dma, dma, dma,
            dma((chunks,)), dma((chunks,)),
            dma((chunks, columns - 1)), dma((chunks, columns - 1)),
            dma((chunks,)), dma((chunks,)),
            dma((chunks, columns - 1)), dma((chunks, columns - 1)),
            dma((chunks,)), dma((chunks,)),
        ],
        compiler_params=pltpu.CompilerParams(
            collective_id=0, has_side_effects=True, vmem_limit_bytes=48 * 1024 * 1024
        ),
    )(q_in, k_in, t_in, w_in)
    return jnp.swapaxes(out.reshape(heads, span, nope), 0, 1)[None]


def body_for(mesh, queries, latent_pages, page_scales, page_table, lengths, w_keys, w_values):
    args = (queries, latent_pages, page_scales, page_table, lengths, w_keys, w_values)
    shards = mesh.shape["ctx"]
    rope = latent_pages.shape[3] - w_keys.shape[0] * shards
    fits = (
        mesh.shape["groups"] == 2 and mesh.shape["head"] == 2 and shards % 2 == 0
        and shards >= 4 and w_keys.shape[0] % 16 == 0 and queries.shape[2] % (2 * PAIR) == 0
        and w_keys.shape == w_values.shape and 2 * rope == w_keys.shape[2]
    )
    if fits:
        return shared_on_device(shards, *args)
    return on_device(*args)


def solution(mesh):
    return jax.shard_map(
        functools.partial(body_for, mesh),
        mesh=mesh,
        in_specs=(
            P(("groups", "ctx"), None, "head", None),
            P(("groups", "ctx"), "head", None, None),
            P(("groups", "ctx"), "head", None, None),
            P(("groups", "ctx"), None),
            P(("groups", "ctx")),
            P("ctx", "head", None),
            P("ctx", "head", None),
        ),
        out_specs=P(("groups", "ctx"), None, "head", None),
        check_vma=False,
    )
```

```python
import functools
import math

import jax
import jax.numpy as jnp
from jax import lax
from jax.experimental import pallas as pl
from jax.experimental.pallas import tpu as pltpu
from jax.sharding import PartitionSpec as P

NEGATIVE = -1e30
MESH = pl.DeviceIdType.MESH
PAIR = 2
LAG = 1


def attend_block(
    running, span_query, page_data, page_factor, first_key, row_offset, up_keys, up_values
):
    row_top, row_total, summed = running
    latent_width = up_keys.shape[0]
    group_count = page_factor.shape[1]
    page_rows = page_data.shape[1]
    key_count = page_data.shape[0] * page_rows
    head_count = span_query.shape[1]
    code_values = page_data[:, :, :latent_width].astype(jnp.float32)
    code_values = code_values.reshape(
        page_data.shape[0], page_rows, group_count, latent_width // group_count
    )
    factor = jnp.swapaxes(page_factor, 1, 2).astype(jnp.float32)[..., None]
    latent = (code_values * factor).reshape(key_count, latent_width).astype(jnp.bfloat16)
    rotary = page_data[:, :, latent_width:].reshape(key_count, -1)
    key_nope = jnp.dot(latent, up_keys, preferred_element_type=jnp.float32).astype(jnp.bfloat16)
    key_nope = key_nope.reshape(key_count, head_count, -1)
    value_rows = jnp.dot(latent, up_values, preferred_element_type=jnp.float32).astype(jnp.bfloat16)
    value_rows = value_rows.reshape(key_count, head_count, -1)
    nope_width = key_nope.shape[2]
    scores = jnp.einsum(
        "chn,khn->hck", span_query[:, :, :nope_width], key_nope, preferred_element_type=jnp.float32
    )
    scores = scores + jnp.einsum(
        "chr,kr->hck", span_query[:, :, nope_width:], rotary, preferred_element_type=jnp.float32
    )
    scores = scores * (1.0 / math.sqrt(span_query.shape[2]))
    row_position = lax.broadcasted_iota(jnp.int32, (span_query.shape[0], key_count), 0)
    key_position = first_key + lax.broadcasted_iota(jnp.int32, (span_query.shape[0], key_count), 1)
    visible = (key_position <= row_offset + row_position)[None]
    new_top = jnp.maximum(row_top, jnp.max(jnp.where(visible, scores, NEGATIVE), axis=2))
    raw_weight = jnp.where(visible, jnp.exp(scores - new_top[..., None]), 0.0)
    rescale = jnp.exp(row_top - new_top)
    row_total = row_total * rescale + jnp.sum(raw_weight, axis=2)
    weights = raw_weight.astype(jnp.bfloat16)
    summed = summed * jnp.swapaxes(rescale, 0, 1)[..., None] + jnp.einsum(
        "hck,khv->chv", weights, value_rows, preferred_element_type=jnp.float32
    )
    return (new_top, row_total, summed)


def sweep(span_query, row_offset, first_block, stop_block, fetch, up_keys, up_values):
    row_count = span_query.shape[0]
    head_count = span_query.shape[1]
    value_width = up_values.shape[1] // head_count
    initial = (
        jnp.full((head_count, row_count), NEGATIVE, jnp.float32),
        jnp.zeros((head_count, row_count), jnp.float32),
        jnp.zeros((row_count, head_count, value_width), jnp.float32),
    )

    def advance(block_index, running):
        page_data, page_factor, first_key = fetch(block_index)
        return attend_block(
            running, span_query, page_data, page_factor, first_key, row_offset, up_keys, up_values
        )

    return lax.fori_loop(first_block, stop_block, advance, initial)


def finish(row_total, summed):
    return (summed / jnp.swapaxes(row_total, 0, 1)[..., None]).astype(jnp.bfloat16)[None]


def on_device(queries, latent_pages, page_scales, page_table, lengths, w_keys, w_values):
    pool_pages, pool_scales = (
        lax.all_gather(latent_pages, "head", axis=1, tiled=True),
        lax.all_gather(page_scales, "head", axis=1, tiled=True),
    )
    full_keys, full_values = (
        lax.all_gather(w_keys, "ctx", axis=0, tiled=True),
        lax.all_gather(w_values, "ctx", axis=0, tiled=True),
    )
    latent_width = full_keys.shape[0]
    up_keys = full_keys.reshape(latent_width, -1)
    up_values = full_values.reshape(latent_width, -1)
    span_query = queries[0]
    own_pages = pool_pages[0]
    own_scales = pool_scales[0]
    own_table = page_table[0]
    row_count = span_query.shape[0]
    block_keys = 2 * own_pages.shape[1]
    own_length = lengths[0]
    block_count = (own_length + block_keys - 1) // block_keys

    def own_fetch(block_index):
        pool_slots = lax.dynamic_slice_in_dim(own_table, 2 * block_index, 2)
        return (
            jnp.take(own_pages, pool_slots, axis=0),
            jnp.take(own_scales, pool_slots, axis=0),
            block_index * block_keys,
        )

    row_top, row_total, summed = sweep(
        span_query, own_length - row_count, 0, block_count, own_fetch, up_keys, up_values
    )
    return finish(row_total, summed)


def gather_attend(
    shard_columns, q_in, k_in, t_in, w_in, out, q_rx, q_own, k_all, t_rx, w_all, rot, late, stage,
    own_sem, core_send, core_recv, relay_send, relay_recv, k_send, k_recv, t_send, t_recv,
    q_send, q_recv, z_send, z_recv, x_send, x_recv, f_send, f_recv,
    r_send, g_send, o_send, o_recv
):
    chunk_count = w_in.shape[1]
    latent_width = w_all.shape[2] * w_all.shape[3]
    span = q_in.shape[-1]
    nope = w_all.shape[-1] // 2
    rope = q_in.shape[-2] - nope
    key_count = k_all.shape[1] * k_all.shape[2]
    scale = 1.0 / math.sqrt(nope + rope)
    y, ctx, core = lax.axis_index("groups"), lax.axis_index("ctx"), lax.axis_index("head")
    row, side = ctx // 2, lax.rem(ctx, 2)
    y_peer = {"groups": 1 - y}
    core_peer = {"head": 1 - core}
    x_peer = {"ctx": 2 * row + 1 - side}

    def z_index(offset):
        return 2 * lax.rem(row + offset, shard_columns) + side

    barrier = pltpu.get_barrier_semaphore()
    peers = [y_peer, core_peer, x_peer] + [{"ctx": z_index(d)} for d in range(1, shard_columns)]
    for peer in peers:
        pl.semaphore_signal(barrier, inc=1, device_id=peer, device_id_type=MESH)
    pl.semaphore_wait(barrier, len(peers))

    def remote(source, target, send, recv, peer):
        return pltpu.make_async_remote_copy(
            src_ref=source, dst_ref=target, send_sem=send, recv_sem=recv,
            device_id=peer, device_id_type=MESH,
        )

    k_copy = remote(k_in, k_all.at[y, core], k_send, k_recv, y_peer)
    t_copy = remote(t_in, t_rx, t_send, t_recv, y_peer)
    core_copy = remote(k_in, k_all.at[y, core], core_send, core_recv, core_peer)
    relay_copy = remote(
        k_all.at[1 - y, core], k_all.at[1 - y, core], relay_send, relay_recv, core_peer
    )
    k_own = pltpu.make_async_copy(k_in, k_all.at[y, core], own_sem.at[0])
    w_own = pltpu.make_async_copy(w_in.at[y], w_all.at[:, :, ctx], own_sem.at[1])

    q_mine = pltpu.make_async_copy(q_in.at[y], q_own, own_sem.at[2])
    last = shard_columns - 1
    relays = jnp.logical_or(row == 1, row == last - 1)
    relay_source = jnp.where(row == 1, last, 0)
    partner = row + 1 - 2 * lax.rem(row, 2)

    def far(other):
        return jnp.abs(other - row) == last

    def block(c, source_row, source_side):
        return w_all.at[c, :, 2 * source_row + source_side]

    def q_copy(c):
        return remote(q_in.at[1 - y, c], q_rx.at[c], q_send.at[c], q_recv.at[c], y_peer)

    def z_copy(c, d):
        return remote(
            w_in.at[y, c], block(c, row, side), z_send.at[c, d - 1], z_recv.at[c, row],
            {"ctx": z_index(d)},
        )

    def z_arrival(c, source):
        return remote(
            w_in.at[y, c], block(c, source, side), z_send.at[c, 0], z_recv.at[c, source], x_peer
        )

    def r_copy(c):
        moved = block(c, relay_source, side)
        return remote(
            moved, moved, r_send.at[c], z_recv.at[c, relay_source],
            {"ctx": 2 * (last - relay_source) + side},
        )

    def x_copy(c):
        return remote(w_in.at[y, c], block(c, row, side), x_send.at[c], x_recv.at[c], x_peer)

    def x_arrival(c):
        return remote(w_in.at[y, c], block(c, row, 1 - side), x_send.at[c], x_recv.at[c], x_peer)

    def f_copy(c, source):
        moved = block(c, source, side)
        return remote(moved, moved, f_send.at[c, source], f_recv.at[c, source], x_peer)

    def f_arrival(c, source):
        moved = block(c, source, 1 - side)
        return remote(moved, moved, f_send.at[c, source], f_recv.at[c, source], x_peer)

    def g_copy(c):
        moved = block(c, row, 1 - side)
        return remote(
            moved, moved, g_send.at[c], f_recv.at[c, row], {"ctx": 2 * partner + side}
        )

    def over_x(c, source):
        return jnp.logical_or(lax.rem(c, 2) == 0, source != partner)

    def o_copy(c):
        return remote(stage.at[c], out.at[y, c], o_send.at[c], o_recv.at[c], y_peer)

    k_copy.start()
    t_copy.start()
    core_copy.start()
    k_own.start()
    q_mine.start()
    w_own.start()

    def begin(c, carry):
        for d in range(1, shard_columns):
            @pl.when(jnp.logical_not(far(lax.rem(row + d, shard_columns))))
            def _():
                z_copy(c, d).start()
        x_copy(c).start()
        q_copy(c).start()
        return carry

    lax.fori_loop(0, chunk_count, begin, 0)
    k_own.wait()
    w_own.wait()
    q_mine.wait()
    k_copy.wait_recv()
    relay_copy.start()
    t_copy.wait_recv()
    core_copy.wait_recv()
    relay_copy.wait_recv()
    page = key_count // t_in.shape[1]
    offset = lax.broadcasted_iota(jnp.int32, (page, span), 0)
    offset = offset - lax.broadcasted_iota(jnp.int32, (page, span), 1)
    for request, t_ref in ((y, t_in), (1 - y, t_rx)):
        rot[request] = k_all[request, :, :, latent_width:].reshape(key_count, rope)
        late[request] = jnp.concatenate(
            [t_ref[0:1, p : p + 1] + offset for p in range(t_in.shape[1])], axis=0
        )

    def attend(c, request, q_ref, put):
        latent = k_all[request, :, :, :latent_width].reshape(key_count, latent_width)
        visible = late[request] <= 0
        for h in range(PAIR):
            weight = w_all[c, h].reshape(latent_width, -1)
            up = jnp.dot(latent, weight, preferred_element_type=jnp.float32).astype(jnp.bfloat16)
            keys = jnp.concatenate([up[:, :nope], rot[request]], axis=1)
            scores = jnp.dot(keys, q_ref[h], preferred_element_type=jnp.float32)
            scores = jnp.where(visible, scores * scale, NEGATIVE)
            top = jnp.max(scores, axis=0, keepdims=True)
            raw = jnp.where(visible, jnp.exp(scores - top), 0.0)
            total = jnp.sum(raw, axis=0, keepdims=True)
            summed = lax.dot_general(
                up[:, nope:], raw.astype(jnp.bfloat16), (((0,), (0,)), ((), ())),
                preferred_element_type=jnp.float32,
            )
            put(h, jnp.transpose(summed / total).astype(jnp.bfloat16))

    def advance(c, carry):
        @pl.when(c < chunk_count)
        def _():
            x_arrival(c).wait_recv()

            @pl.when(lax.rem(c, 2) == 1)
            def _():
                g_copy(c).start()

            for d in range(1, shard_columns):
                source = lax.rem(row + d, shard_columns)
                z_arrival(c, source).wait_recv()

                @pl.when(jnp.logical_and(relays, source == relay_source))
                def _():
                    r_copy(c).start()

                @pl.when(over_x(c, source))
                def _():
                    f_copy(c, source).start()

        @pl.when(c >= LAG)
        def _():
            b = c - LAG
            for d in range(1, shard_columns):
                f_arrival(b, lax.rem(row + d, shard_columns)).wait_recv()
            q_copy(b).wait_recv()

            def put_stage(h, value):
                stage[b, h] = value

            def put_out(h, value):
                out[y, b, h] = value

            attend(b, 1 - y, q_rx.at[b], put_stage)
            attend(b, y, q_own.at[b], put_out)
            o_copy(b).start()

        return carry

    lax.fori_loop(0, chunk_count + LAG, advance, 0)
    k_copy.wait_send()
    t_copy.wait_send()
    core_copy.wait_send()
    relay_copy.wait_send()

    def end(c, carry):
        q_copy(c).wait_send()
        x_copy(c).wait_send()
        for d in range(1, shard_columns):
            other = lax.rem(row + d, shard_columns)

            @pl.when(jnp.logical_not(far(other)))
            def _():
                z_copy(c, d).wait_send()

            @pl.when(over_x(c, other))
            def _():
                f_copy(c, other).wait_send()

        @pl.when(relays)
        def _():
            r_copy(c).wait_send()

        @pl.when(lax.rem(c, 2) == 1)
        def _():
            g_copy(c).wait_send()

        o_copy(c).wait()
        return carry

    lax.fori_loop(0, chunk_count, end, 0)


def shared_on_device(
    shards, queries, latent_pages, page_scales, page_table, lengths, w_keys, w_values
):
    _, span, heads, _ = queries.shape
    latent_rows, _, nope = w_keys.shape
    _, slots, page, width = latent_pages.shape
    latent_width = latent_rows * shards
    rope = width - latent_width
    groups = page_scales.shape[2]
    chunks = heads // (2 * PAIR)
    keys = slots * page
    columns = shards // 2
    w_in = jnp.concatenate([jnp.swapaxes(w_keys, 0, 1), jnp.swapaxes(w_values, 0, 1)], axis=-1)
    w_in = w_in.reshape(2, chunks, PAIR, latent_rows, 2 * nope)
    q_in = jnp.transpose(queries[0], (1, 2, 0)).reshape(2, chunks, PAIR, -1, span)
    codes = latent_pages[0, :, :, :latent_width].astype(jnp.float32)
    codes = codes.reshape(slots, page, groups, latent_width // groups)
    factor = jnp.swapaxes(page_scales[0], 1, 2).astype(jnp.float32)[..., None]
    latent = (codes * factor).reshape(keys, latent_width).astype(jnp.bfloat16)
    rotary = latent_pages[0, :, :, latent_width:].reshape(keys, rope)
    k_in = jnp.concatenate([latent, rotary], axis=1)
    pool = page_table.shape[1]
    places = jnp.arange(pool, dtype=jnp.int32)
    order = jnp.sum(jnp.where(page_table[0][:, None] == places[None], places[:, None], 0), axis=0)
    t_in = jnp.broadcast_to((order * page - (lengths[0] - span))[None], (8, pool))
    dma, vmem = pltpu.SemaphoreType.DMA, pltpu.VMEM
    bf16 = jnp.bfloat16
    out = pl.pallas_call(
        functools.partial(gather_attend, columns),
        out_shape=jax.ShapeDtypeStruct((2, chunks, PAIR, span, nope), bf16),
        in_specs=[pl.BlockSpec(memory_space=pl.ANY)] + [pl.BlockSpec(memory_space=vmem)] * 3,
        out_specs=pl.BlockSpec(memory_space=vmem),
        scratch_shapes=[
            vmem(q_in.shape[1:], bf16),
            vmem(q_in.shape[1:], bf16),
            vmem((2, 2, keys, k_in.shape[1]), bf16),
            vmem(t_in.shape, jnp.int32),
            vmem((chunks, PAIR, shards, latent_rows, 2 * nope), bf16),
            vmem((2, 2 * keys, rope), bf16),
            vmem((2, 2 * keys, span), jnp.int32),
            vmem((chunks, PAIR, span, nope), bf16),
            dma((3,)), dma, dma, dma, dma, dma, dma, dma, dma,
            dma((chunks,)), dma((chunks,)),
            dma((chunks, columns - 1)), dma((chunks, columns)),
            dma((chunks,)), dma((chunks,)),
            dma((chunks, columns)), dma((chunks, columns)),
            dma((chunks,)), dma((chunks,)), dma((chunks,)), dma((chunks,)),
        ],
        compiler_params=pltpu.CompilerParams(
            collective_id=0, has_side_effects=True, vmem_limit_bytes=48 * 1024 * 1024
        ),
    )(q_in, k_in, t_in, w_in)
    return jnp.swapaxes(out.reshape(heads, span, nope), 0, 1)[None]


def body_for(mesh, queries, latent_pages, page_scales, page_table, lengths, w_keys, w_values):
    args = (queries, latent_pages, page_scales, page_table, lengths, w_keys, w_values)
    shards = mesh.shape["ctx"]
    rope = latent_pages.shape[3] - w_keys.shape[0] * shards
    fits = (
        mesh.shape["groups"] == 2 and mesh.shape["head"] == 2 and shards % 4 == 0
        and shards >= 8 and w_keys.shape[0] % 16 == 0 and queries.shape[2] % (2 * PAIR) == 0
        and w_keys.shape == w_values.shape and 2 * rope == w_keys.shape[2]
    )
    if fits:
        return shared_on_device(shards, *args)
    return on_device(*args)


def solution(mesh):
    return jax.shard_map(
        functools.partial(body_for, mesh),
        mesh=mesh,
        in_specs=(
            P(("groups", "ctx"), None, "head", None),
            P(("groups", "ctx"), "head", None, None),
            P(("groups", "ctx"), "head", None, None),
            P(("groups", "ctx"), None),
            P(("groups", "ctx")),
            P("ctx", "head", None),
            P("ctx", "head", None),
        ),
        out_specs=P(("groups", "ctx"), None, "head", None),
        check_vma=False,
    )
```

```python
import functools
import math

import jax
import jax.numpy as jnp
from jax import lax
from jax.experimental import pallas as pl
from jax.experimental.pallas import tpu as pltpu
from jax.sharding import PartitionSpec as P

NEGATIVE = -1e30
MESH = pl.DeviceIdType.MESH
PAIR = 4
LAG = 1


def attend_block(
    running, span_query, page_data, page_factor, first_key, row_offset, up_keys, up_values
):
    row_top, row_total, summed = running
    latent_width = up_keys.shape[0]
    group_count = page_factor.shape[1]
    page_rows = page_data.shape[1]
    key_count = page_data.shape[0] * page_rows
    head_count = span_query.shape[1]
    code_values = page_data[:, :, :latent_width].astype(jnp.float32)
    code_values = code_values.reshape(
        page_data.shape[0], page_rows, group_count, latent_width // group_count
    )
    factor = jnp.swapaxes(page_factor, 1, 2).astype(jnp.float32)[..., None]
    latent = (code_values * factor).reshape(key_count, latent_width).astype(jnp.bfloat16)
    rotary = page_data[:, :, latent_width:].reshape(key_count, -1)
    key_nope = jnp.dot(latent, up_keys, preferred_element_type=jnp.float32).astype(jnp.bfloat16)
    key_nope = key_nope.reshape(key_count, head_count, -1)
    value_rows = jnp.dot(latent, up_values, preferred_element_type=jnp.float32).astype(jnp.bfloat16)
    value_rows = value_rows.reshape(key_count, head_count, -1)
    nope_width = key_nope.shape[2]
    scores = jnp.einsum(
        "chn,khn->hck", span_query[:, :, :nope_width], key_nope, preferred_element_type=jnp.float32
    )
    scores = scores + jnp.einsum(
        "chr,kr->hck", span_query[:, :, nope_width:], rotary, preferred_element_type=jnp.float32
    )
    scores = scores * (1.0 / math.sqrt(span_query.shape[2]))
    row_position = lax.broadcasted_iota(jnp.int32, (span_query.shape[0], key_count), 0)
    key_position = first_key + lax.broadcasted_iota(jnp.int32, (span_query.shape[0], key_count), 1)
    visible = (key_position <= row_offset + row_position)[None]
    new_top = jnp.maximum(row_top, jnp.max(jnp.where(visible, scores, NEGATIVE), axis=2))
    raw_weight = jnp.where(visible, jnp.exp(scores - new_top[..., None]), 0.0)
    rescale = jnp.exp(row_top - new_top)
    row_total = row_total * rescale + jnp.sum(raw_weight, axis=2)
    weights = raw_weight.astype(jnp.bfloat16)
    summed = summed * jnp.swapaxes(rescale, 0, 1)[..., None] + jnp.einsum(
        "hck,khv->chv", weights, value_rows, preferred_element_type=jnp.float32
    )
    return (new_top, row_total, summed)


def sweep(span_query, row_offset, first_block, stop_block, fetch, up_keys, up_values):
    row_count = span_query.shape[0]
    head_count = span_query.shape[1]
    value_width = up_values.shape[1] // head_count
    initial = (
        jnp.full((head_count, row_count), NEGATIVE, jnp.float32),
        jnp.zeros((head_count, row_count), jnp.float32),
        jnp.zeros((row_count, head_count, value_width), jnp.float32),
    )

    def advance(block_index, running):
        page_data, page_factor, first_key = fetch(block_index)
        return attend_block(
            running, span_query, page_data, page_factor, first_key, row_offset, up_keys, up_values
        )

    return lax.fori_loop(first_block, stop_block, advance, initial)


def finish(row_total, summed):
    return (summed / jnp.swapaxes(row_total, 0, 1)[..., None]).astype(jnp.bfloat16)[None]


def on_device(queries, latent_pages, page_scales, page_table, lengths, w_keys, w_values):
    pool_pages, pool_scales = (
        lax.all_gather(latent_pages, "head", axis=1, tiled=True),
        lax.all_gather(page_scales, "head", axis=1, tiled=True),
    )
    full_keys, full_values = (
        lax.all_gather(w_keys, "ctx", axis=0, tiled=True),
        lax.all_gather(w_values, "ctx", axis=0, tiled=True),
    )
    latent_width = full_keys.shape[0]
    up_keys = full_keys.reshape(latent_width, -1)
    up_values = full_values.reshape(latent_width, -1)
    span_query = queries[0]
    own_pages = pool_pages[0]
    own_scales = pool_scales[0]
    own_table = page_table[0]
    row_count = span_query.shape[0]
    block_keys = 2 * own_pages.shape[1]
    own_length = lengths[0]
    block_count = (own_length + block_keys - 1) // block_keys

    def own_fetch(block_index):
        pool_slots = lax.dynamic_slice_in_dim(own_table, 2 * block_index, 2)
        return (
            jnp.take(own_pages, pool_slots, axis=0),
            jnp.take(own_scales, pool_slots, axis=0),
            block_index * block_keys,
        )

    row_top, row_total, summed = sweep(
        span_query, own_length - row_count, 0, block_count, own_fetch, up_keys, up_values
    )
    return finish(row_total, summed)


def gather_attend(
    shard_columns, q_in, k_in, t_in, w_in, out, q_rx, q_own, k_all, t_rx, w_all, rot, late, stage,
    own_sem, core_send, core_recv, relay_send, relay_recv, k_send, k_recv, t_send, t_recv,
    q_send, q_recv, z_send, z_recv, x_send, x_recv, f_send, f_recv,
    r_send, g_send, o_send, o_recv
):
    chunk_count = w_in.shape[1]
    latent_width = w_all.shape[2] * w_all.shape[3]
    span = q_in.shape[-1]
    nope = w_all.shape[-1] // 2
    rope = q_in.shape[-2] - nope
    key_count = k_all.shape[1] * k_all.shape[2]
    scale = 1.0 / math.sqrt(nope + rope)
    y, ctx, core = lax.axis_index("groups"), lax.axis_index("ctx"), lax.axis_index("head")
    row, side = ctx // 2, lax.rem(ctx, 2)
    y_peer = {"groups": 1 - y}
    core_peer = {"head": 1 - core}
    x_peer = {"ctx": 2 * row + 1 - side}

    def z_index(offset):
        return 2 * lax.rem(row + offset, shard_columns) + side

    barrier = pltpu.get_barrier_semaphore()
    peers = [y_peer, core_peer, x_peer] + [{"ctx": z_index(d)} for d in range(1, shard_columns)]
    for peer in peers:
        pl.semaphore_signal(barrier, inc=1, device_id=peer, device_id_type=MESH)
    pl.semaphore_wait(barrier, len(peers))

    def remote(source, target, send, recv, peer):
        return pltpu.make_async_remote_copy(
            src_ref=source, dst_ref=target, send_sem=send, recv_sem=recv,
            device_id=peer, device_id_type=MESH,
        )

    k_copy = remote(k_in, k_all.at[y, core], k_send, k_recv, y_peer)
    t_copy = remote(t_in, t_rx, t_send, t_recv, y_peer)
    core_copy = remote(k_in, k_all.at[y, core], core_send, core_recv, core_peer)
    relay_copy = remote(
        k_all.at[1 - y, core], k_all.at[1 - y, core], relay_send, relay_recv, core_peer
    )
    k_own = pltpu.make_async_copy(k_in, k_all.at[y, core], own_sem.at[0])
    w_own = pltpu.make_async_copy(w_in.at[y], w_all.at[:, :, ctx], own_sem.at[1])

    q_mine = pltpu.make_async_copy(q_in.at[y], q_own, own_sem.at[2])
    last = shard_columns - 1
    partner = row + 1 - 2 * lax.rem(row, 2)

    others = [row + step * d for d in range(1, shard_columns) for step in (1, -1)]

    def exists(other):
        return jnp.logical_and(other >= 0, other <= last)

    def onward(source):
        return jnp.where(source < row, row + 1, row - 1)

    def block(c, source_row, source_side):
        return w_all.at[c, :, 2 * source_row + source_side]

    def q_copy(c):
        return remote(q_in.at[1 - y, c], q_rx.at[c], q_send.at[c], q_recv.at[c], y_peer)

    def z_copy(c, step):
        return remote(
            w_in.at[y, c], block(c, row, side), z_send.at[c, (step + 1) // 2], z_recv.at[c, row],
            {"ctx": 2 * (row + step) + side},
        )

    def z_arrival(c, source):
        return remote(
            w_in.at[y, c], block(c, source, side), z_send.at[c, 0], z_recv.at[c, source], x_peer
        )

    def r_copy(c, source):
        moved = block(c, source, side)
        return remote(
            moved, moved, r_send.at[c, source], z_recv.at[c, source],
            {"ctx": 2 * onward(source) + side},
        )

    def x_copy(c):
        return remote(w_in.at[y, c], block(c, row, side), x_send.at[c], x_recv.at[c], x_peer)

    def x_arrival(c):
        return remote(w_in.at[y, c], block(c, row, 1 - side), x_send.at[c], x_recv.at[c], x_peer)

    def f_copy(c, source):
        moved = block(c, source, side)
        return remote(moved, moved, f_send.at[c, source], f_recv.at[c, source], x_peer)

    def f_arrival(c, source):
        moved = block(c, source, 1 - side)
        return remote(moved, moved, f_send.at[c, source], f_recv.at[c, source], x_peer)

    def g_copy(c):
        moved = block(c, row, 1 - side)
        return remote(
            moved, moved, g_send.at[c], f_recv.at[c, row], {"ctx": 2 * partner + side}
        )

    def over_x(c, source):
        return jnp.logical_or(lax.rem(c, 2) == 0, source != partner)

    def o_copy(c):
        return remote(stage.at[c], out.at[y, c], o_send.at[c], o_recv.at[c], y_peer)

    k_copy.start()
    t_copy.start()
    core_copy.start()
    k_own.start()
    q_mine.start()
    w_own.start()

    def begin(c, carry):
        for step in (1, -1):
            @pl.when(exists(row + step))
            def _():
                z_copy(c, step).start()

        x_copy(c).start()
        q_copy(c).start()
        return carry

    lax.fori_loop(0, chunk_count, begin, 0)
    k_own.wait()
    w_own.wait()
    q_mine.wait()
    def settle():
        t_copy.wait_recv()
        core_copy.wait_recv()
        relay_copy.wait_recv()
        page = key_count // t_in.shape[1]
        offset = lax.broadcasted_iota(jnp.int32, (page, span), 0)
        offset = offset - lax.broadcasted_iota(jnp.int32, (page, span), 1)
        for request, t_ref in ((y, t_in), (1 - y, t_rx)):
            rot[request] = k_all[request, :, :, latent_width:].reshape(key_count, rope)
            late[request] = jnp.concatenate(
                [t_ref[0:1, p : p + 1] + offset for p in range(t_in.shape[1])], axis=0
            )

    def attend(c, request, q_ref, put):
        latent = k_all[request, :, :, :latent_width].reshape(key_count, latent_width)
        visible = late[request] <= 0
        for h in range(PAIR):
            weight = w_all[c, h].reshape(latent_width, -1)
            up = jnp.dot(latent, weight, preferred_element_type=jnp.float32).astype(jnp.bfloat16)
            keys = jnp.concatenate([up[:, :nope], rot[request]], axis=1)
            scores = jnp.dot(keys, q_ref[h], preferred_element_type=jnp.float32)
            scores = jnp.where(visible, scores * scale, NEGATIVE)
            top = jnp.max(scores, axis=0, keepdims=True)
            raw = jnp.where(visible, jnp.exp(scores - top), 0.0)
            total = jnp.sum(raw, axis=0, keepdims=True)
            summed = lax.dot_general(
                up[:, nope:], raw.astype(jnp.bfloat16), (((0,), (0,)), ((), ())),
                preferred_element_type=jnp.float32,
            )
            put(h, jnp.transpose(summed / total).astype(jnp.bfloat16))

    def advance(c, carry):
        @pl.when(c < chunk_count)
        def _():
            x_arrival(c).wait_recv()

            @pl.when(lax.rem(c, 2) == 1)
            def _():
                g_copy(c).start()

            for source in others:
                @pl.when(exists(source))
                def _():
                    z_arrival(c, source).wait_recv()

                    @pl.when(exists(onward(source)))
                    def _():
                        r_copy(c, source).start()

                    @pl.when(over_x(c, source))
                    def _():
                        f_copy(c, source).start()

        @pl.when(c == 0)
        def _():
            k_copy.wait_recv()
            relay_copy.start()

        @pl.when(c == LAG)
        def _():
            settle()

        @pl.when(c >= LAG)
        def _():
            b = c - LAG
            for d in range(1, shard_columns):
                f_arrival(b, lax.rem(row + d, shard_columns)).wait_recv()
            q_copy(b).wait_recv()

            def put_stage(h, value):
                stage[b, h] = value

            def put_out(h, value):
                out[y, b, h] = value

            attend(b, 1 - y, q_rx.at[b], put_stage)
            attend(b, y, q_own.at[b], put_out)
            o_copy(b).start()

        return carry

    lax.fori_loop(0, chunk_count + LAG, advance, 0)
    k_copy.wait_send()
    t_copy.wait_send()
    core_copy.wait_send()
    relay_copy.wait_send()

    def end(c, carry):
        q_copy(c).wait_send()
        x_copy(c).wait_send()
        for d in range(1, shard_columns):
            other = lax.rem(row + d, shard_columns)

            @pl.when(over_x(c, other))
            def _():
                f_copy(c, other).wait_send()

            @pl.when(exists(onward(other)))
            def _():
                r_copy(c, other).wait_send()

        for step in (1, -1):
            @pl.when(exists(row + step))
            def _():
                z_copy(c, step).wait_send()

        @pl.when(lax.rem(c, 2) == 1)
        def _():
            g_copy(c).wait_send()

        o_copy(c).wait()
        return carry

    lax.fori_loop(0, chunk_count, end, 0)


def shared_on_device(
    shards, queries, latent_pages, page_scales, page_table, lengths, w_keys, w_values
):
    _, span, heads, _ = queries.shape
    latent_rows, _, nope = w_keys.shape
    _, slots, page, width = latent_pages.shape
    latent_width = latent_rows * shards
    rope = width - latent_width
    groups = page_scales.shape[2]
    chunks = heads // (2 * PAIR)
    keys = slots * page
    columns = shards // 2
    w_in = jnp.concatenate([jnp.swapaxes(w_keys, 0, 1), jnp.swapaxes(w_values, 0, 1)], axis=-1)
    w_in = w_in.reshape(2, chunks, PAIR, latent_rows, 2 * nope)
    q_in = jnp.transpose(queries[0], (1, 2, 0)).reshape(2, chunks, PAIR, -1, span)
    codes = latent_pages[0, :, :, :latent_width].astype(jnp.float32)
    codes = codes.reshape(slots, page, groups, latent_width // groups)
    factor = jnp.swapaxes(page_scales[0], 1, 2).astype(jnp.float32)[..., None]
    latent = (codes * factor).reshape(keys, latent_width).astype(jnp.bfloat16)
    rotary = latent_pages[0, :, :, latent_width:].reshape(keys, rope)
    k_in = jnp.concatenate([latent, rotary], axis=1)
    pool = page_table.shape[1]
    places = jnp.arange(pool, dtype=jnp.int32)
    order = jnp.sum(jnp.where(page_table[0][:, None] == places[None], places[:, None], 0), axis=0)
    t_in = jnp.broadcast_to((order * page - (lengths[0] - span))[None], (8, pool))
    dma, vmem = pltpu.SemaphoreType.DMA, pltpu.VMEM
    bf16 = jnp.bfloat16
    out = pl.pallas_call(
        functools.partial(gather_attend, columns),
        out_shape=jax.ShapeDtypeStruct((2, chunks, PAIR, span, nope), bf16),
        in_specs=[pl.BlockSpec(memory_space=pl.ANY)] + [pl.BlockSpec(memory_space=vmem)] * 3,
        out_specs=pl.BlockSpec(memory_space=vmem),
        scratch_shapes=[
            vmem(q_in.shape[1:], bf16),
            vmem(q_in.shape[1:], bf16),
            vmem((2, 2, keys, k_in.shape[1]), bf16),
            vmem(t_in.shape, jnp.int32),
            vmem((chunks, PAIR, shards, latent_rows, 2 * nope), bf16),
            vmem((2, 2 * keys, rope), bf16),
            vmem((2, 2 * keys, span), jnp.int32),
            vmem((chunks, PAIR, span, nope), bf16),
            dma((3,)), dma, dma, dma, dma, dma, dma, dma, dma,
            dma((chunks,)), dma((chunks,)),
            dma((chunks, 2)), dma((chunks, columns)),
            dma((chunks,)), dma((chunks,)),
            dma((chunks, columns)), dma((chunks, columns)),
            dma((chunks, columns)), dma((chunks,)), dma((chunks,)), dma((chunks,)),
        ],
        compiler_params=pltpu.CompilerParams(
            collective_id=0, has_side_effects=True, vmem_limit_bytes=48 * 1024 * 1024
        ),
    )(q_in, k_in, t_in, w_in)
    return jnp.swapaxes(out.reshape(heads, span, nope), 0, 1)[None]


def body_for(mesh, queries, latent_pages, page_scales, page_table, lengths, w_keys, w_values):
    args = (queries, latent_pages, page_scales, page_table, lengths, w_keys, w_values)
    shards = mesh.shape["ctx"]
    rope = latent_pages.shape[3] - w_keys.shape[0] * shards
    fits = (
        mesh.shape["groups"] == 2 and mesh.shape["head"] == 2 and shards % 4 == 0
        and shards >= 8 and w_keys.shape[0] % 16 == 0 and queries.shape[2] % (2 * PAIR) == 0
        and w_keys.shape == w_values.shape and 2 * rope == w_keys.shape[2]
    )
    if fits:
        return shared_on_device(shards, *args)
    return on_device(*args)


def solution(mesh):
    return jax.shard_map(
        functools.partial(body_for, mesh),
        mesh=mesh,
        in_specs=(
            P(("groups", "ctx"), None, "head", None),
            P(("groups", "ctx"), "head", None, None),
            P(("groups", "ctx"), "head", None, None),
            P(("groups", "ctx"), None),
            P(("groups", "ctx")),
            P("ctx", "head", None),
            P("ctx", "head", None),
        ),
        out_specs=P(("groups", "ctx"), None, "head", None),
        check_vma=False,
    )
```
